256 devices in a mesh: tm: 2 (over y_lo), row: 16 (over y_hi, z), col: 8 (over x, core).
Axes of the slice: x: 4, y: 4 (y_hi: 2, y_lo: 2; y = y_hi * 2 + y_lo), z: 8, core: 2. Of those that a mesh axis runs over, the one named last changes fastest.
Arguments:
- returns: bfloat16 [272, 16384], P('tm', ('row', 'col')), may hold values from -60 to 60
- window: int32 [1], replicated, may hold values from 200 to 256
- out_days: int32 [4], replicated, may hold values from 255 to 271
Outputs:
- correlation: bfloat16 [4, 16384, 16384], P(None, 'row', ('col', 'tm'))
The draws below stay inside these ranges and needn't reach their ends.
Inputs may be any that keep to these rules, and one draw needn't show every extreme that they name: One window length for all days. `out_days`: days may repeat.
All inputs are finite; a program needn't handle non-finite values.
Results may differ from the reference program's by a relative error of at most 0.001.
Values may be sent and summed in bfloat16 or wider, within the bound.
No kernel may reach another device: no remote copies, remote signals or barrier semaphores. Data moves between devices by JAX's collectives and lax.ppermute only.
A program may use at most 128 MiB of HBM per device.

```python
import jax
import jax.numpy as jnp
from jax import lax

ASSETS = 16384
DAYS = 272
NOUT = 4


def draw_returns(key, part):
    keys = jax.random.split(jax.random.fold_in(key, 17), 5)
    day_scale = jnp.exp(jax.random.uniform(keys[0], (DAYS, 1), jnp.float32, jnp.log(0.3), jnp.log(3.0)))
    asset_scale = jnp.exp(jax.random.uniform(keys[1], (1, ASSETS), jnp.float32, jnp.log(0.5), jnp.log(5.0)))
    loading = jax.random.uniform(keys[2], (1, ASSETS), jnp.float32, 0.4, 1.6)
    market = jax.random.normal(keys[3], (DAYS, 1), jnp.float32)
    noise = jax.random.normal(keys[4], (DAYS, ASSETS), jnp.float32)
    signal = loading * market + noise
    values = jnp.clip(day_scale * asset_scale * signal, -60.0, 60.0)
    return values.astype(jnp.bfloat16)


def plant(entries, key, smallest, top_value):
    extent = entries.shape
    place = [jax.random.randint(jax.random.fold_in(key, axis), (), 0, extent[axis]) for axis in range(len(extent))]
    entries = entries.at[tuple(place)].set(smallest)
    longest = extent.index(max(extent))
    place[longest] = (place[longest] + 1) % extent[longest]
    return entries.at[tuple(place)].set(top_value)


def setup_inputs(seed: int = 0) -> dict:
    streams_of = jax.random.split(jax.random.key(seed), 4)
    return {
        "returns": draw_returns(jax.random.fold_in(streams_of[3], 71), 0),
        "window": jax.random.randint(streams_of[1], (1,), 200, 257).astype(jnp.int32),
        "out_days": plant(jax.random.randint(streams_of[2], (NOUT,), 255, DAYS), jax.random.fold_in(streams_of[2], 1), 255, DAYS - 1).astype(jnp.int32),
    }


def reference(returns, window, out_days):
    width = window[0]
    wide = width.astype(jnp.float32)
    day_ids = jnp.arange(DAYS, dtype=jnp.int32)
    inside = (day_ids[None, :] <= out_days[:, None]) & (day_ids[None, :] > out_days[:, None] - width)
    mask = jnp.where(inside, 1.0, 0.0).astype(jnp.float32)
    series = returns.astype(jnp.float32)
    first = jnp.dot(mask, series, precision=lax.Precision.HIGHEST)
    second = jnp.dot(mask, series * series, precision=lax.Precision.HIGHEST)
    scale = lax.rsqrt((second - first * first / wide) / wide + 1e-06)
    blocks = ASSETS // 512

    def one_block(index):
        start = (index * 512).astype(jnp.int32)
        rows = lax.dynamic_slice_in_dim(series, start, 512, 1)
        weighted = mask[:, :, None] * rows[None, :, :]
        gram = jnp.einsum('kda,db->kab', weighted, series, precision=lax.Precision.HIGHEST)
        first_rows = lax.dynamic_slice_in_dim(first, start, 512, 1)
        scale_rows = lax.dynamic_slice_in_dim(scale, start, 512, 1)
        cov = gram - first_rows[:, :, None] * first[:, None, :] / wide
        return (cov * scale_rows[:, :, None] * scale[:, None, :] / wide).astype(jnp.bfloat16)
    pieces = lax.map(one_block, jnp.arange(blocks, dtype=jnp.int32))
    return jnp.transpose(pieces, (1, 0, 2, 3)).reshape(NOUT, ASSETS, ASSETS)
```

```python
import functools
import itertools

import jax
import jax.numpy as jnp
from jax import lax
from jax.experimental import pallas as pl
from jax.experimental.pallas import tpu as pltpu
from jax.sharding import Mesh
from jax.sharding import PartitionSpec as P

AXES = ("yl", "yh", "zh", "zq", "x", "c")
SIZES = (2, 2, 2, 4, 4, 2)
LANES = 128


def place(yl, yh, zh, zq, x, c):
    number = 0
    for size, index in zip(SIZES, (yl, yh, zh, zq, x, c)):
        number = number * size + index
    return number


def corner_turn():
    pairs = []
    for yl, yh, zh, zq, x, c in itertools.product(*map(range, SIZES)):
        to_x, to_c, to_yl = 2 * yh + zh, zq // 2, zq % 2
        to_yh = yh if yl == to_yl else 1 - yh
        to = (to_yl, to_yh, c, (zq + x - to_x) % 4, to_x, to_c)
        pairs.append((place(yl, yh, zh, zq, x, c), place(*to)))
    return pairs


def ring(size, step):
    return [(i, (i + step) % size) for i in range(size)]


def two_apart(size):
    return [(i, (i + 2 - 4 * (i % 2)) % size) for i in range(size)]


def days_by_assets(block):
    columns = [
        jnp.concatenate([block[h, c].astype(jnp.float32) for h in range(2)], axis=0) for c in range(2)
    ]
    return jnp.concatenate(columns, axis=1)


def statistics(series, facts, k):
    width, last = facts[0], facts[1 + k]
    wide = width.astype(jnp.float32)
    day = lax.broadcasted_iota(jnp.int32, series.shape, 0)
    kept = jnp.where((day <= last) & (day > last - width), series, 0.0)
    first = jnp.sum(kept, axis=0, keepdims=True)
    second = jnp.sum(kept * kept, axis=0, keepdims=True)
    scale = lax.rsqrt((second - first * first / wide) / wide + 1e-06)
    return first, scale, wide


def prepare_rows(facts, own, before, after, across, left, stats):
    x = lax.axis_index("x")
    for ref, step in ((own, 0), (before, 3), (after, 1), (across, 2)):
        quarter = lax.rem(x + step, 4)
        rows = pl.ds(pl.multiple_of(quarter * 256, 256), 256)
        series = days_by_assets(ref)
        days, assets = series.shape
        spare = days - 256
        main = series[:256].T
        folded = jnp.concatenate([series[256:], jnp.zeros((LANES - spare, assets), jnp.float32)], axis=0).T
        columns = []
        for k in range(4):
            first, scale, _ = statistics(series, facts, k)
            columns.append((first, scale))
            width, last = facts[0], facts[1 + k]
            slot = lax.broadcasted_iota(jnp.int32, (assets, LANES), 1)
            low = jnp.where(slot > last - width, main[:, :LANES], 0.0)
            low = jnp.where((slot < spare) & (slot + 256 <= last), folded, low)
            left[k, rows, :LANES] = low.astype(jnp.bfloat16)
            left[k, rows, LANES:] = jnp.where(
                slot + LANES > last - width, main[:, LANES:], 0.0
            ).astype(jnp.bfloat16)
        table = [first for first, _ in columns] + [scale for _, scale in columns]
        table.append(jnp.zeros((LANES - 8, assets), jnp.float32))
        stats[rows, :] = jnp.concatenate(table, axis=0).T


def quarter_of_columns(step, facts, left, stats, block, *rest):
    out, result, sems = rest[-3:]
    turn = lax.axis_index("x") + lax.axis_index("zq") - 2 * lax.axis_index("c") - lax.axis_index("yl")
    quarter = lax.rem(turn + step + 8, 4)
    columns = pl.ds(pl.multiple_of(quarter * 256, 256), 256)
    series = days_by_assets(block)
    spare = series.shape[0] - 256
    common = series[spare:256].astype(jnp.bfloat16)
    copies = []
    for k in range(4):
        first, scale, wide = statistics(series, facts, k)
        mean, scale = first / wide, scale / wide
        slot = lax.broadcasted_iota(jnp.int32, (spare, series.shape[1]), 0)
        head = jnp.where(slot + 256 <= facts[1 + k], series[256:], series[:spare])
        right = jnp.concatenate([head.astype(jnp.bfloat16), common], axis=0)
        for i in range(4):
            rows = slice(i * 256, (i + 1) * 256)
            gram = jnp.dot(left[k, rows, :], right, preferred_element_type=jnp.float32)
            cov = gram - stats[rows, k : k + 1] * mean
            result[k, rows, :] = (cov * stats[rows, 4 + k : 5 + k] * scale).astype(jnp.bfloat16)
        copy = pltpu.make_async_copy(result.at[k], out.at[k, :, columns], sems.at[k])
        copy.start()
        copies.append(copy)
    for copy in copies:
        copy.wait()


def on_device(returns, window, out_days):
    facts = jnp.concatenate([window, out_days])
    pair = lax.all_gather(returns, "c", axis=0)
    turned = lax.ppermute(pair, AXES, corner_turn())
    own_rows = lax.all_gather(pair, "yl", axis=0)
    rows = [own_rows]
    for links in (ring(4, 1), ring(4, 3), ring(4, 2)):
        rows.append(lax.ppermute(own_rows, "x", links))
    other = lax.ppermute(turned, "yh", ring(2, 1))
    half = lax.axis_index("yl") + lax.axis_index("yh") + lax.axis_index("x") // 2
    own_columns = jnp.where(half % 2 == 0, jnp.stack([turned, other]), jnp.stack([other, turned]))
    columns = [(0, own_columns)]
    for step, links in ((3, ring(8, 1)), (1, ring(8, 7)), (2, two_apart(8))):
        columns.append((step, lax.ppermute(own_columns, ("zh", "zq"), links)))

    smem, vmem = pl.BlockSpec(memory_space=pltpu.SMEM), pl.BlockSpec(memory_space=pltpu.VMEM)
    anywhere = pl.BlockSpec(memory_space=pl.ANY)
    assets = 1024
    left, stats = pl.pallas_call(
        prepare_rows,
        out_shape=(
            jax.ShapeDtypeStruct((4, assets, 256), jnp.bfloat16),
            jax.ShapeDtypeStruct((assets, LANES), jnp.float32),
        ),
        in_specs=[smem] + [vmem] * 4,
        out_specs=(vmem, vmem),
        cost_estimate=pl.CostEstimate(flops=2_000_000_000, bytes_accessed=4_000_000, transcendentals=0),
        name="prepare_rows",
    )(facts, *rows)
    out = None
    for step, block in columns:
        out = pl.pallas_call(
            functools.partial(quarter_of_columns, step),
            out_shape=jax.ShapeDtypeStruct((4, assets, assets), jnp.bfloat16),
            in_specs=[smem, vmem, vmem, vmem] + ([anywhere] if out is not None else []),
            out_specs=anywhere,
            scratch_shapes=[pltpu.VMEM((4, assets, 256), jnp.bfloat16), pltpu.SemaphoreType.DMA((4,))],
            input_output_aliases={} if out is None else {4: 0},
            cost_estimate=pl.CostEstimate(flops=2_000_000_000, bytes_accessed=4_000_000, transcendentals=0),
            name="quarter",
        )(*([facts, left, stats, block] + ([out] if out is not None else [])))
    return out


def solution(mesh):
    fine = Mesh(mesh.devices.reshape(SIZES), AXES)
    return jax.shard_map(
        on_device,
        mesh=fine,
        in_specs=(P("yl", ("yh", "zh", "zq", "x", "c")), P(), P()),
        out_specs=P(None, ("yh", "zh", "zq"), ("x", "c", "yl")),
        check_vma=False,
    )
```

```python
import functools
import itertools

import jax
import jax.numpy as jnp
from jax import lax
from jax.experimental import pallas as pl
from jax.experimental.pallas import tpu as pltpu
from jax.sharding import Mesh
from jax.sharding import PartitionSpec as P

AXES = ("yl", "yh", "zh", "zq", "x", "c")
SIZES = (2, 2, 2, 4, 4, 2)
LANES = 128
DEPTH = 256
EARLY = 72
CHUNK = 512
CALLS = (((0,), slice(0, 1)), ((3, 1, 2), slice(1, 4)))
PARAMS = pltpu.CompilerParams(vmem_limit_bytes=24 * 2**20)


def place(yl, yh, zh, zq, x, c):
    number = 0
    for size, index in zip(SIZES, (yl, yh, zh, zq, x, c)):
        number = number * size + index
    return number


def corner_turn():
    pairs = []
    for yl, yh, zh, zq, x, c in itertools.product(*map(range, SIZES)):
        to_x, to_c, to_yl = 2 * yh + zh, zq // 2, zq % 2
        to_yh = yh if yl == to_yl else 1 - yh
        to_zh = (c + zh + to_c + 1) % 2
        to = (to_yl, to_yh, to_zh, (zq + x - to_x) % 4, to_x, to_c)
        pairs.append((place(yl, yh, zh, zq, x, c), place(*to)))
    assert all(source != target for source, target in pairs)
    return pairs


def ring(size, step):
    return [(i, (i + step) % size) for i in range(size)]


def two_apart(size):
    return [(i, (i + 2 - 4 * (i % 2)) % size) for i in range(size)]


def days_by_assets(block):
    columns = [
        jnp.concatenate([block[h, c].astype(jnp.float32) for h in range(2)], axis=0) for c in range(2)
    ]
    return jnp.concatenate(columns, axis=1)


def total(series):
    return jnp.sum(series, axis=0, keepdims=True)


def statistics(series, width, lasts):
    wide = width.astype(jnp.float32)
    middle, early, late = series[EARLY:DEPTH], series[:EARLY], series[DEPTH:]
    first_middle, second_middle = total(middle), total(middle * middle)
    early_day = lax.broadcasted_iota(jnp.int32, early.shape, 0)
    late_day = lax.broadcasted_iota(jnp.int32, late.shape, 0) + DEPTH
    found = []
    for last in lasts:
        kept_early = jnp.where(early_day > last - width, early, 0.0)
        kept_late = jnp.where(late_day <= last, late, 0.0)
        first = first_middle + total(kept_early) + total(kept_late)
        second = second_middle + total(kept_early * kept_early) + total(kept_late * kept_late)
        found.append((first, lax.rsqrt((second - first * first / wide) / wide + 1e-06)))
    return found


def encoded(window, out_days):
    late = jnp.sum(lax.shift_left(out_days - (DEPTH - 1), 5 * jnp.arange(4, dtype=jnp.int32) + 9))
    return (window[0] + late).reshape(1)


def decoded(facts):
    code = facts[0]
    lasts = [(lax.shift_right_logical(code, 9 + 5 * k) & 31) + (DEPTH - 1) for k in range(4)]
    return code & 511, lasts


def prepare_rows(facts, own, before, after, across, low, high, spread):
    width, lasts = decoded(facts)
    x = lax.axis_index("x")
    for ref, step in ((own, 0), (before, 3), (after, 1), (across, 2)):
        quarter = lax.rem(x + step, 4)
        rows = pl.ds(pl.multiple_of(quarter * 256, 256), 256)
        series = days_by_assets(ref)
        days, assets = series.shape
        spare = days - DEPTH
        found = statistics(series, width, lasts)
        table = [first for first, _ in found] + [scale for _, scale in found]
        table.append(jnp.zeros((LANES - 8, assets), jnp.float32))
        stats = jnp.concatenate(table, axis=0).T
        for n in range(8):
            spread[n, rows, :] = jnp.broadcast_to(stats[:, n : n + 1], (assets, LANES))
        high[rows, :] = series[LANES:DEPTH].T.astype(jnp.bfloat16)
        main = series[:LANES].T
        folded = jnp.concatenate([series[DEPTH:], jnp.zeros((LANES - spare, assets), jnp.float32)], axis=0).T
        slot = lax.broadcasted_iota(jnp.int32, (assets, LANES), 1)
        for k, last in enumerate(lasts):
            left = jnp.where(slot > last - width, main, 0.0)
            left = jnp.where((slot < spare) & (slot + DEPTH <= last), folded, left)
            low[k, rows, :] = left.astype(jnp.bfloat16)


def correlate(steps, facts, low, high, spread, *refs):
    blocks, (out, result, sems) = refs[: len(steps)], refs[-3:]
    turn = lax.axis_index("x") + lax.axis_index("zq") - 2 * lax.axis_index("c") - lax.axis_index("yl")
    width, lasts = decoded(facts)
    wide = width.astype(jnp.float32)
    copies = []
    for n, (step, block) in enumerate(zip(steps, blocks)):
        columns = pl.ds(pl.multiple_of(lax.rem(turn + step + 8, 4) * 256, 256), 256)
        series = days_by_assets(block)
        spare = series.shape[0] - DEPTH
        common = series[spare:DEPTH].astype(jnp.bfloat16)
        for k, (first, scale) in enumerate(statistics(series, width, lasts)):
            mean, scale = first / wide, scale / wide
            slot = lax.broadcasted_iota(jnp.int32, (spare, series.shape[1]), 0)
            head = jnp.where(slot + DEPTH <= lasts[k], series[DEPTH:], series[:spare])
            right = jnp.concatenate([head.astype(jnp.bfloat16), common], axis=0)
            for i in range(low.shape[1] // CHUNK):
                rows = slice(i * CHUNK, (i + 1) * CHUNK)
                left = jnp.concatenate([low[k, rows, :], high[rows, :]], axis=1)
                gram = jnp.dot(left, right, preferred_element_type=jnp.float32)
                row_sum, row_scale = spread[k, rows, :], spread[4 + k, rows, :]
                for h in (slice(0, LANES), slice(LANES, 2 * LANES)):
                    cov = gram[:, h] - row_sum * mean[:, h]
                    result[n, k, rows, h] = (cov * row_scale * scale[:, h]).astype(jnp.bfloat16)
                copy = pltpu.make_async_copy(
                    result.at[n, k, rows], out.at[k, rows, columns], sems.at[n, k, i]
                )
                copy.start()
                copies.append(copy)
    for copy in copies:
        copy.wait()


def exchange_and_correlate(returns, window, out_days):
    facts = encoded(window, out_days)
    pair = lax.all_gather(returns, "c", axis=0)
    turned = lax.ppermute(pair, AXES, corner_turn())
    own_rows = lax.all_gather(pair, "yl", axis=0)
    turned, own_rows = lax.optimization_barrier((turned, own_rows))
    other = lax.ppermute(turned, "yh", ring(2, 1))
    rows = [own_rows]
    for links in (ring(4, 1), ring(4, 3), ring(4, 2)):
        rows.append(lax.ppermute(own_rows, "x", links))
    half = lax.axis_index("yl") + lax.axis_index("yh") + lax.axis_index("x") // 2
    own_columns = jnp.where(half % 2 == 0, jnp.stack([turned, other]), jnp.stack([other, turned]))
    columns = [own_columns]
    for links in (ring(8, 1), ring(8, 7), two_apart(8)):
        columns.append(lax.ppermute(own_columns, ("zh", "zq"), links))

    smem, vmem = pl.BlockSpec(memory_space=pltpu.SMEM), pl.BlockSpec(memory_space=pltpu.VMEM)
    anywhere = pl.BlockSpec(memory_space=pl.ANY)
    assets = 1024
    prepared = pl.pallas_call(
        prepare_rows,
        out_shape=(
            jax.ShapeDtypeStruct((4, assets, LANES), jnp.bfloat16),
            jax.ShapeDtypeStruct((assets, LANES), jnp.bfloat16),
            jax.ShapeDtypeStruct((8, assets, LANES), jnp.float32),
        ),
        in_specs=[smem] + [vmem] * 4,
        out_specs=(vmem, vmem, vmem),
        cost_estimate=pl.CostEstimate(flops=2_000_000_000, bytes_accessed=4_000_000, transcendentals=0),
        compiler_params=PARAMS,
        name="prepare_rows",
    )(facts, *rows)
    out = []
    for steps, blocks in CALLS:
        count = len(steps)
        out = [
            pl.pallas_call(
                functools.partial(correlate, steps),
                out_shape=jax.ShapeDtypeStruct((4, assets, assets), jnp.bfloat16),
                in_specs=[smem] + [vmem] * (3 + count) + [anywhere] * len(out),
                out_specs=anywhere,
                scratch_shapes=[
                    pltpu.VMEM((count, 4, assets, 256), jnp.bfloat16),
                    pltpu.SemaphoreType.DMA((count, 4, assets // CHUNK)),
                ],
                input_output_aliases={4 + count: 0} if out else {},
                cost_estimate=pl.CostEstimate(
                    flops=2_000_000_000 * count, bytes_accessed=2_000_000 * count, transcendentals=0
                ),
                compiler_params=PARAMS,
                name="correlate",
            )(facts, *prepared, *columns[blocks], *out)
        ]
    return out[0]


def solution(mesh):
    fine = Mesh(mesh.devices.reshape(SIZES), AXES)
    return jax.shard_map(
        exchange_and_correlate,
        mesh=fine,
        in_specs=(P("yl", ("yh", "zh", "zq", "x", "c")), P(), P()),
        out_specs=P(None, ("yh", "zh", "zq"), ("x", "c", "yl")),
        check_vma=False,
    )
```

```python
import functools
import itertools

import jax
import jax.numpy as jnp
from jax import lax
from jax.experimental import pallas as pl
from jax.experimental.pallas import tpu as pltpu
from jax.sharding import Mesh
from jax.sharding import PartitionSpec as P

AXES = ("yl", "yh", "zh", "zq", "x", "c")
SIZES = (2, 2, 2, 4, 4, 2)
LANES = 128
DEPTH = 256
EARLY = 72
LATE = 16
CHUNK = 512
CALLS = (("across",), ("after", "before"))
PARAMS = pltpu.CompilerParams(vmem_limit_bytes=24 * 2**20)


def place(yl, yh, zh, zq, x, c):
    number = 0
    for size, index in zip(SIZES, (yl, yh, zh, zq, x, c)):
        number = number * size + index
    return number


def corner_turn():
    pairs = []
    for yl, yh, zh, zq, x, c in itertools.product(*map(range, SIZES)):
        to_x, to_c, to_yl = 2 * yh + zh, zq // 2, zq % 2
        to_yh = (yh + (yl != to_yl)) % 2
        to_zh = (c + zh + to_c + 1) % 2
        to = (to_yl, to_yh, to_zh, (zq + x - to_x) % 4, to_x, to_c)
        pairs.append((place(yl, yh, zh, zq, x, c), place(*to)))
    assert all(source != target for source, target in pairs)
    return pairs


def ring(size, step):
    return [(i, (i + step) % size) for i in range(size)]


def two_apart(size):
    return [(i, (i + 2 - 4 * (i % 2)) % size) for i in range(size)]


def write_masks(window, out_days, mask):
    width = window[0]
    early = lax.broadcasted_iota(jnp.int32, (EARLY, LANES), 0)
    late = lax.broadcasted_iota(jnp.int32, (LATE, LANES), 0) + DEPTH
    slot = lax.broadcasted_iota(jnp.int32, (1, LANES), 1)
    base = 4 * (EARLY + LATE)

    def one(test):
        return jnp.where(test, 1.0, 0.0).astype(jnp.float32)

    for k in range(4):
        last, start = out_days[k], k * (EARLY + LATE)
        mask[start : start + EARLY, :] = one(early > last - width)
        mask[start + EARLY : start + EARLY + LATE, :] = one(late <= last)
        mask[base + k : base + k + 1, :] = one(slot > last - width)
        mask[base + 4 + k : base + 5 + k, :] = one((slot < LATE) & (slot + DEPTH <= last))
    mask[base + 8 :, :] = jnp.full((8, LANES), width.astype(jnp.float32))


def twice(tile):
    return jnp.concatenate([tile, tile], axis=1)


def total(series):
    return jnp.sum(series, axis=0, keepdims=True)


def days_by_assets(block, half, chunk):
    columns = []
    for i in range(2):
        parts = [block[lax.rem(half + h, 2), lax.rem(chunk + i, 2)].astype(jnp.float32) for h in range(2)]
        columns.append(jnp.concatenate(parts, axis=0))
    return jnp.concatenate(columns, axis=1)


def by_day(mask, k):
    return mask[k * (EARLY + LATE) : (k + 1) * (EARLY + LATE), :]


def by_slot(mask, n):
    return mask[4 * (EARLY + LATE) + n : 4 * (EARLY + LATE) + n + 1, :]


def statistics(series, mask, wide):
    middle, early, late = series[EARLY:DEPTH], series[:EARLY], series[DEPTH:]
    first_middle, second_middle = total(middle), total(middle * middle)
    found = []
    for k in range(4):
        days = twice(by_day(mask, k))
        kept_early, kept_late = early * days[:EARLY], late * days[EARLY:]
        first = first_middle + total(kept_early) + total(kept_late)
        second = second_middle + total(kept_early * kept_early) + total(kept_late * kept_late)
        found.append((first, lax.rsqrt((second - first * first / wide) / wide + 1e-06)))
    return found


def along_lanes(table):
    high = table.astype(jnp.bfloat16)
    rest = table - high.astype(jnp.float32)
    middle = rest.astype(jnp.bfloat16)
    low = (rest - middle.astype(jnp.float32)).astype(jnp.bfloat16)
    parts = jnp.concatenate([part.astype(jnp.float32) for part in (high, middle, low)] + [jnp.zeros_like(table)], axis=0)
    row = lax.broadcasted_iota(jnp.int32, (4 * 8, 8 * LANES), 0)
    lane = lax.broadcasted_iota(jnp.int32, (4 * 8, 8 * LANES), 1)
    ones = jnp.where(row % 8 == lane // LANES, 1.0, 0.0).astype(jnp.bfloat16)
    return lax.dot_general(
        parts.astype(jnp.bfloat16), ones, (((0,), (0,)), ((), ())), preferred_element_type=jnp.float32
    )


def prepare_rows(mask, blocks, low, high, spread):
    x, c, yl = lax.axis_index("x"), lax.axis_index("c"), lax.axis_index("yl")
    wide = twice(by_slot(mask, 8))
    for step, block in zip((0, 3, 1, 2), blocks):
        rows = pl.ds(pl.multiple_of(lax.rem(x + step, 4) * 256, 256), 256)
        series = days_by_assets(block, yl, c)
        assets = series.shape[1]
        found = statistics(series, mask, wide)
        turned = along_lanes(jnp.concatenate([first for first, _ in found] + [scale for _, scale in found], axis=0))
        for i in range(8):
            spread[i, rows, :] = turned[:, i * LANES : (i + 1) * LANES]
        high[rows, :] = series[LANES:DEPTH].T.astype(jnp.bfloat16)
        main = series[:LANES].T
        folded = jnp.concatenate([series[DEPTH:], jnp.zeros((LANES - LATE, assets), jnp.float32)], axis=0).T
        for k in range(4):
            left = jnp.where(by_slot(mask, 4 + k) > 0.5, folded, main * by_slot(mask, k))
            low[k, rows, :] = left.astype(jnp.bfloat16)


def correlate(block, source, mask, low, high, spread, finish):
    x, c, yl, yh = (lax.axis_index(name) for name in ("x", "c", "yl", "yh"))
    z = 4 * lax.axis_index("zh") + lax.axis_index("zq")
    away = {"own": 0, "before": 7, "after": 1, "across": 6 - 4 * lax.rem(z, 2)}[source]
    half = lax.rem(yl + yh + x // 2, 2)
    from_core = lax.rem(lax.rem(z + away + 8, 8) // 4 + x + c + 1, 2)
    wide = twice(by_slot(mask, 8))
    series = days_by_assets(block, half, from_core)
    common = series[LATE:DEPTH].astype(jnp.bfloat16)
    for k, (first, scale) in enumerate(statistics(series, mask, wide)):
        mean, scale = first / wide, scale / wide
        head = jnp.where(twice(by_day(mask, k)[EARLY:]) > 0.5, series[DEPTH:], series[:LATE])
        right = jnp.concatenate([head.astype(jnp.bfloat16), common], axis=0)
        for i in range(low.shape[1] // CHUNK):
            rows = slice(i * CHUNK, (i + 1) * CHUNK)
            left = jnp.concatenate([low[k, rows, :], high[rows, :]], axis=1)
            gram = jnp.dot(left, right, preferred_element_type=jnp.float32)
            row_sum, row_scale = spread[k, rows, :], spread[4 + k, rows, :]
            tiles = []
            for h in (slice(0, LANES), slice(LANES, 2 * LANES)):
                cov = gram[:, h] - row_sum * mean[:, h]
                tiles.append((cov * row_scale * scale[:, h]).astype(jnp.bfloat16))
            finish(k, i, rows, tiles)


def columns_of(source):
    x, c, yl, zq = (lax.axis_index(name) for name in ("x", "c", "yl", "zq"))
    step = {"own": 0, "before": 3, "after": 1, "across": 2}[source]
    return pl.ds(pl.multiple_of(lax.rem(x + zq - 2 * c - yl + step + 8, 4) * 256, 256), 256)


def store(result, k, rows, tiles):
    for n, tile in enumerate(tiles):
        result[k, rows, n * LANES : (n + 1) * LANES] = tile


def begin(mask, own, before, after, across, own_block, low, high, spread, result):
    prepare_rows(mask, (own, before, after, across), low, high, spread)

    def finish(k, i, rows, tiles):
        store(result, k, rows, tiles)

    correlate(own_block, "own", mask, low, high, spread, finish)


def go_on(sources, ready, mask, low, high, spread, *refs):
    count = len(sources)
    blocks, (out, result, sems) = refs[:count], refs[-3:]
    copies = []

    def send(block, number, k, i, rows, source):
        copy = pltpu.make_async_copy(block.at[k, rows], out.at[k, rows, columns_of(source)], sems.at[number, k, i])
        copy.start()
        copies.append(copy)

    if ready is not None:
        for k in range(4):
            for i in range(low.shape[1] // CHUNK):
                send(refs[count], count, k, i, slice(i * CHUNK, (i + 1) * CHUNK), ready)
    for n, (source, block) in enumerate(zip(sources, blocks)):

        def finish(k, i, rows, tiles, n=n, source=source):
            store(result.at[n], k, rows, tiles)
            send(result.at[n], n, k, i, rows, source)

        correlate(block, source, mask, low, high, spread, finish)
    for copy in copies:
        copy.wait()


def exchange_and_correlate(returns, window, out_days):
    vmem, anywhere = pl.BlockSpec(memory_space=pltpu.VMEM), pl.BlockSpec(memory_space=pl.ANY)
    assets = 1024
    smem = pl.BlockSpec(memory_space=pltpu.SMEM)
    mask = pl.pallas_call(
        write_masks,
        out_shape=jax.ShapeDtypeStruct((4 * (EARLY + LATE) + 16, LANES), jnp.float32),
        in_specs=[smem, smem],
        out_specs=vmem,
        cost_estimate=pl.CostEstimate(flops=1_000_000_000, bytes_accessed=200_000, transcendentals=0),
        compiler_params=PARAMS,
        name="write_masks",
    )(window, out_days)
    pair = jnp.stack([returns, lax.ppermute(returns, "c", ring(2, 1))])
    turned = lax.ppermute(pair, AXES, corner_turn())
    own_rows = jnp.stack([pair, lax.ppermute(pair, "yl", ring(2, 1))])
    other = lax.ppermute(turned, "yh", ring(2, 1))
    rows = [own_rows]
    for links in (ring(4, 1), ring(4, 3), ring(4, 2)):
        rows.append(lax.ppermute(own_rows, "x", links))
    own = jnp.stack([turned, other])
    quarters = {"own": own}
    for source, links in (("before", ring(8, 1)), ("after", ring(8, 7)), ("across", two_apart(8))):
        quarters[source] = lax.ppermute(own, ("zh", "zq"), links)

    *prepared, own_result = pl.pallas_call(
        begin,
        out_shape=(
            jax.ShapeDtypeStruct((4, assets, LANES), jnp.bfloat16),
            jax.ShapeDtypeStruct((assets, LANES), jnp.bfloat16),
            jax.ShapeDtypeStruct((8, assets, LANES), jnp.float32),
            jax.ShapeDtypeStruct((4, assets, 256), jnp.bfloat16),
        ),
        in_specs=[vmem] * 6,
        out_specs=(vmem,) * 4,
        cost_estimate=pl.CostEstimate(flops=4_000_000_000, bytes_accessed=4_000_000, transcendentals=0),
        compiler_params=PARAMS,
        name="begin",
    )(mask, *rows, own)
    out, ready = [], "own"
    for sources in CALLS:
        count = len(sources)
        held = [] if ready is None else [own_result]
        out = [
            pl.pallas_call(
                functools.partial(go_on, sources, ready),
                out_shape=jax.ShapeDtypeStruct((4, assets, assets), jnp.bfloat16),
                in_specs=[vmem] * (4 + count + len(held)) + [anywhere] * len(out),
                out_specs=anywhere,
                scratch_shapes=[
                    pltpu.VMEM((count, 4, assets, 256), jnp.bfloat16),
                    pltpu.SemaphoreType.DMA((count + len(held), 4, assets // CHUNK)),
                ],
                input_output_aliases={4 + count: 0} if out else {},
                cost_estimate=pl.CostEstimate(
                    flops=2_000_000_000 * count, bytes_accessed=2_000_000 * count, transcendentals=0
                ),
                compiler_params=PARAMS,
                name="go_on",
            )(mask, *prepared, *[quarters[source] for source in sources], *held, *out)
        ]
        ready = None
    return out[0]


def solution(mesh):
    fine = Mesh(mesh.devices.reshape(SIZES), AXES)
    return jax.shard_map(
        exchange_and_correlate,
        mesh=fine,
        in_specs=(P("yl", ("yh", "zh", "zq", "x", "c")), P(), P()),
        out_specs=P(None, ("yh", "zh", "zq"), ("x", "c", "yl")),
        check_vma=False,
    )
```

```python
import functools
import itertools

import jax
import jax.numpy as jnp
from jax import lax
from jax.experimental import pallas as pl
from jax.experimental.pallas import tpu as pltpu
from jax.sharding import Mesh
from jax.sharding import PartitionSpec as P

AXES = ("yl", "yh", "zh", "zq", "x", "c")
SIZES = (2, 2, 2, 4, 4, 2)
LANES = 128
DEPTH = 256
EARLY = 72
LATE = 16
CHUNK = 512
ORDER = ("before", "across", "after")
CALLS = (ORDER[:1], ORDER[1:])
PARAMS = pltpu.CompilerParams(vmem_limit_bytes=24 * 2**20)


def place(yl, yh, zh, zq, x, c):
    number = 0
    for size, index in zip(SIZES, (yl, yh, zh, zq, x, c)):
        number = number * size + index
    return number


def corner_turn():
    pairs = []
    for yl, yh, zh, zq, x, c in itertools.product(*map(range, SIZES)):
        to_x, to_c, to_yl = 2 * yh + zh, zq // 2, zq % 2
        to_yh = (yh + (yl != to_yl)) % 2
        to_zh = (c + zh + to_c + 1) % 2
        to = (to_yl, to_yh, to_zh, (zq + x - to_x) % 4, to_x, to_c)
        pairs.append((place(yl, yh, zh, zq, x, c), place(*to)))
    assert all(source != target for source, target in pairs)
    return pairs


def ring(size, step):
    return [(i, (i + step) % size) for i in range(size)]


def two_apart(size):
    return [(i, (i + 2 - 4 * (i % 2)) % size) for i in range(size)]


def write_masks(window, out_days, mask):
    width = window[0]
    early = lax.broadcasted_iota(jnp.int32, (EARLY, LANES), 0)
    late = lax.broadcasted_iota(jnp.int32, (LATE, LANES), 0) + DEPTH
    slot = lax.broadcasted_iota(jnp.int32, (1, LANES), 1)
    base = 4 * (EARLY + LATE)

    def one(test):
        return jnp.where(test, 1.0, 0.0).astype(jnp.float32)

    for k in range(4):
        last, start = out_days[k], k * (EARLY + LATE)
        mask[start : start + EARLY, :] = one(early > last - width)
        mask[start + EARLY : start + EARLY + LATE, :] = one(late <= last)
        mask[base + k : base + k + 1, :] = one(slot > last - width)
        mask[base + 4 + k : base + 5 + k, :] = one((slot < LATE) & (slot + DEPTH <= last))
    mask[base + 8 :, :] = jnp.full((8, LANES), width.astype(jnp.float32))


def twice(tile):
    return jnp.concatenate([tile, tile], axis=1)


def total(series):
    return jnp.sum(series, axis=0, keepdims=True)


def days_by_assets(block, half):
    columns = []
    for chunk in range(2):
        parts = [block[lax.rem(half + h, 2), chunk].astype(jnp.float32) for h in range(2)]
        columns.append(jnp.concatenate(parts, axis=0))
    return jnp.concatenate(columns, axis=1)


def by_day(mask, k):
    return mask[k * (EARLY + LATE) : (k + 1) * (EARLY + LATE), :]


def by_slot(mask, n):
    return mask[4 * (EARLY + LATE) + n : 4 * (EARLY + LATE) + n + 1, :]


def statistics(series, mask, wide):
    middle, early, late = series[EARLY:DEPTH], series[:EARLY], series[DEPTH:]
    first_middle, second_middle = total(middle), total(middle * middle)
    found = []
    for k in range(4):
        days = twice(by_day(mask, k))
        kept_early, kept_late = early * days[:EARLY], late * days[EARLY:]
        first = first_middle + total(kept_early) + total(kept_late)
        second = second_middle + total(kept_early * kept_early) + total(kept_late * kept_late)
        found.append((first, lax.rsqrt((second - first * first / wide) / wide + 1e-06)))
    return found


def along_lanes(table):
    high = table.astype(jnp.bfloat16)
    rest = table - high.astype(jnp.float32)
    middle = rest.astype(jnp.bfloat16)
    low = (rest - middle.astype(jnp.float32)).astype(jnp.bfloat16)
    parts = jnp.concatenate([part.astype(jnp.float32) for part in (high, middle, low)] + [jnp.zeros_like(table)], axis=0)
    row = lax.broadcasted_iota(jnp.int32, (4 * 8, 8 * LANES), 0)
    lane = lax.broadcasted_iota(jnp.int32, (4 * 8, 8 * LANES), 1)
    ones = jnp.where(row % 8 == lane // LANES, 1.0, 0.0).astype(jnp.bfloat16)
    return lax.dot_general(
        parts.astype(jnp.bfloat16), ones, (((0,), (0,)), ((), ())), preferred_element_type=jnp.float32
    )


def prepare_rows(mask, blocks, low, high, spread):
    x, yl = lax.axis_index("x"), lax.axis_index("yl")
    wide = twice(by_slot(mask, 8))
    for step, block in zip((0, 3, 1, 2), blocks):
        rows = pl.ds(pl.multiple_of(lax.rem(x + step, 4) * 256, 256), 256)
        series = days_by_assets(block, yl)
        assets = series.shape[1]
        found = statistics(series, mask, wide)
        turned = along_lanes(jnp.concatenate([first for first, _ in found] + [scale for _, scale in found], axis=0))
        for i in range(8):
            spread[i, rows, :] = turned[:, i * LANES : (i + 1) * LANES]
        high[rows, :] = series[LANES:DEPTH].T.astype(jnp.bfloat16)
        main = series[:LANES].T
        folded = jnp.concatenate([series[DEPTH:], jnp.zeros((LANES - LATE, assets), jnp.float32)], axis=0).T
        for k in range(4):
            left = jnp.where(by_slot(mask, 4 + k) > 0.5, folded, main * by_slot(mask, k))
            low[k, rows, :] = left.astype(jnp.bfloat16)


def correlate(block, mask, low, high, spread, finish):
    half = lax.rem(lax.axis_index("yl") + lax.axis_index("yh") + lax.axis_index("x") // 2, 2)
    wide = twice(by_slot(mask, 8))
    series = days_by_assets(block, half)
    common = series[LATE:DEPTH].astype(jnp.bfloat16)
    for k, (first, scale) in enumerate(statistics(series, mask, wide)):
        mean, scale = first / wide, scale / wide
        head = jnp.where(twice(by_day(mask, k)[EARLY:]) > 0.5, series[DEPTH:], series[:LATE])
        right = jnp.concatenate([head.astype(jnp.bfloat16), common], axis=0)
        for i in range(low.shape[1] // CHUNK):
            rows = slice(i * CHUNK, (i + 1) * CHUNK)
            left = jnp.concatenate([low[k, rows, :], high[rows, :]], axis=1)
            gram = jnp.dot(left, right, preferred_element_type=jnp.float32)
            row_sum, row_scale = spread[k, rows, :], spread[4 + k, rows, :]
            tiles = []
            for h in (slice(0, LANES), slice(LANES, 2 * LANES)):
                cov = gram[:, h] - row_sum * mean[:, h]
                tiles.append((cov * row_scale * scale[:, h]).astype(jnp.bfloat16))
            finish(k, i, rows, tiles)


def columns_of(source):
    x, c, yl, zq = (lax.axis_index(name) for name in ("x", "c", "yl", "zq"))
    step = {"own": 0, "before": 3, "after": 1, "across": 2}[source]
    return pl.ds(pl.multiple_of(lax.rem(x + zq - 2 * c - yl + step + 8, 4) * 256, 256), 256)


def store(result, k, rows, tiles):
    for n, tile in enumerate(tiles):
        result[k, rows, n * LANES : (n + 1) * LANES] = tile


def begin(mask, own, before, after, across, own_block, low, high, spread, result):
    prepare_rows(mask, (own, before, after, across), low, high, spread)

    def finish(k, i, rows, tiles):
        store(result, k, rows, tiles)

    correlate(own_block, mask, low, high, spread, finish)


def go_on(sources, ready, kept, mask, low, high, spread, *refs):
    count = len(sources)
    blocks, held, out = refs[:count], refs[count], refs[-3 - (kept is not None)]
    result, sems = refs[-2:]
    copies = []

    def send(block, number, k, i, rows, source):
        copy = pltpu.make_async_copy(block.at[k, rows], out.at[k, rows, columns_of(source)], sems.at[number, k, i])
        copy.start()
        copies.append(copy)

    for k in range(4):
        for i in range(low.shape[1] // CHUNK):
            send(held, count, k, i, slice(i * CHUNK, (i + 1) * CHUNK), ready)

    def work():
        for n, (source, block) in enumerate(zip(sources, blocks)):

            def finish(k, i, rows, tiles, n=n, source=source):
                store(refs[-3] if source == kept else result.at[n], k, rows, tiles)
                if source != kept:
                    send(result.at[n], n, k, i, rows, source)

            correlate(block, mask, low, high, spread, finish)

    if kept is None:
        work()
    else:
        pl.when(lax.axis_index("x") >= 0)(work)
    for copy in copies:
        copy.wait()


def exchange_and_correlate(returns, window, out_days):
    vmem, anywhere = pl.BlockSpec(memory_space=pltpu.VMEM), pl.BlockSpec(memory_space=pl.ANY)
    assets = 1024
    smem = pl.BlockSpec(memory_space=pltpu.SMEM)
    mask = pl.pallas_call(
        write_masks,
        out_shape=jax.ShapeDtypeStruct((4 * (EARLY + LATE) + 16, LANES), jnp.float32),
        in_specs=[smem, smem],
        out_specs=vmem,
        cost_estimate=pl.CostEstimate(flops=1_000_000_000, bytes_accessed=200_000, transcendentals=0),
        compiler_params=PARAMS,
        name="write_masks",
    )(window, out_days)
    pair = lax.all_gather(returns, "c", axis=0)
    turned = lax.ppermute(pair, AXES, corner_turn())
    own_rows = jnp.stack([pair, lax.ppermute(pair, "yl", ring(2, 1))])
    other = lax.ppermute(turned, "yh", ring(2, 1))
    rows = [own_rows]
    for links in (ring(4, 1), ring(4, 3), ring(4, 2)):
        rows.append(lax.ppermute(own_rows, "x", links))
    own = jnp.stack([turned, other])
    quarters = {"own": own}
    for source, links in (("before", ring(8, 1)), ("after", ring(8, 7)), ("across", two_apart(8))):
        quarters[source] = lax.ppermute(own, ("zh", "zq"), links)

    *prepared, own_result = pl.pallas_call(
        begin,
        out_shape=(
            jax.ShapeDtypeStruct((4, assets, LANES), jnp.bfloat16),
            jax.ShapeDtypeStruct((assets, LANES), jnp.bfloat16),
            jax.ShapeDtypeStruct((8, assets, LANES), jnp.float32),
            jax.ShapeDtypeStruct((4, assets, 256), jnp.bfloat16),
        ),
        in_specs=[vmem] * 6,
        out_specs=(vmem,) * 4,
        cost_estimate=pl.CostEstimate(flops=4_000_000_000, bytes_accessed=4_000_000, transcendentals=0),
        compiler_params=PARAMS,
        name="begin",
    )(mask, *rows, own)
    quarter = jax.ShapeDtypeStruct((4, assets, 256), jnp.bfloat16)
    whole = jax.ShapeDtypeStruct((4, assets, assets), jnp.bfloat16)
    out, ready, held = [], "own", own_result
    for number, sources in enumerate(CALLS):
        count, last = len(sources), number + 1 == len(CALLS)
        out = pl.pallas_call(
            functools.partial(go_on, sources, ready, None if last else sources[-1]),
            out_shape=(whole,) if last else (whole, quarter),
            in_specs=[vmem] * (5 + count) + [anywhere] * len(out),
            out_specs=(anywhere,) if last else (anywhere, vmem),
            scratch_shapes=[
                pltpu.VMEM((count, 4, assets, 256), jnp.bfloat16),
                pltpu.SemaphoreType.DMA((count + 1, 4, assets // CHUNK)),
            ],
            input_output_aliases={5 + count: 0} if out else {},
            cost_estimate=pl.CostEstimate(
                flops=2_000_000_000 * count, bytes_accessed=2_000_000 * count, transcendentals=0
            ),
            compiler_params=PARAMS,
            name="go_on",
        )(mask, *prepared, *[quarters[source] for source in sources], held, *out)
        ready, out, held = sources[-1], out[:1], out[-1]
    return out[0]


def solution(mesh):
    fine = Mesh(mesh.devices.reshape(SIZES), AXES)
    return jax.shard_map(
        exchange_and_correlate,
        mesh=fine,
        in_specs=(P("yl", ("yh", "zh", "zq", "x", "c")), P(), P()),
        out_specs=P(None, ("yh", "zh", "zq"), ("x", "c", "yl")),
        check_vma=False,
    )
```

```python
import functools
import itertools

import jax
import jax.numpy as jnp
from jax import lax
from jax.experimental import pallas as pl
from jax.experimental.pallas import tpu as pltpu
from jax.sharding import Mesh
from jax.sharding import PartitionSpec as P

AXES = ("yl", "yh", "zh", "zq", "x", "c")
SIZES = (2, 2, 2, 4, 4, 2)
LANES = 128
DEPTH = 256
EARLY = 72
LATE = 16
CHUNK = 512
ORDER = ("before", "across", "after")
CALLS = (ORDER[:1], ORDER[1:])
GRANT = 24 * 2**20
PARAMS = pltpu.CompilerParams(vmem_limit_bytes=GRANT)


def place(yl, yh, zh, zq, x, c):
    number = 0
    for size, index in zip(SIZES, (yl, yh, zh, zq, x, c)):
        number = number * size + index
    return number


def corner_turn():
    pairs = []
    for yl, yh, zh, zq, x, c in itertools.product(*map(range, SIZES)):
        to_x, to_c, to_yl = 2 * yh + zh, zq // 2, zq % 2
        to_yh = (yh + (yl != to_yl)) % 2
        to_zh = (c + zh + to_c + 1) % 2
        to = (to_yl, to_yh, to_zh, (zq + x - to_x) % 4, to_x, to_c)
        pairs.append((place(yl, yh, zh, zq, x, c), place(*to)))
    assert all(source != target for source, target in pairs)
    return pairs


def ring(size, step):
    return [(i, (i + step) % size) for i in range(size)]


def two_apart(size):
    return [(i, (i + 2 - 4 * (i % 2)) % size) for i in range(size)]


def write_masks(window, out_days, mask):
    width = window[0]
    early = lax.broadcasted_iota(jnp.int32, (EARLY, LANES), 0)
    late = lax.broadcasted_iota(jnp.int32, (LATE, LANES), 0) + DEPTH
    slot = lax.broadcasted_iota(jnp.int32, (1, LANES), 1)
    base = 4 * (EARLY + LATE)

    def one(test):
        return jnp.where(test, 1.0, 0.0).astype(jnp.float32)

    for k in range(4):
        last, start = out_days[k], k * (EARLY + LATE)
        mask[start : start + EARLY, :] = one(early > last - width)
        mask[start + EARLY : start + EARLY + LATE, :] = one(late <= last)
        mask[base + k : base + k + 1, :] = one(slot > last - width)
        mask[base + 4 + k : base + 5 + k, :] = one((slot < LATE) & (slot + DEPTH <= last))
    mask[base + 8 :, :] = jnp.full((8, LANES), width.astype(jnp.float32))


def twice(tile):
    return jnp.concatenate([tile, tile], axis=1)


def total(series):
    return jnp.sum(series, axis=0, keepdims=True)


def days_by_assets(block, half):
    columns = []
    for chunk in range(2):
        parts = [block[lax.rem(half + h, 2), chunk].astype(jnp.float32) for h in range(2)]
        columns.append(jnp.concatenate(parts, axis=0))
    return jnp.concatenate(columns, axis=1)


def by_day(mask, k):
    return mask[k * (EARLY + LATE) : (k + 1) * (EARLY + LATE), :]


def by_slot(mask, n):
    return mask[4 * (EARLY + LATE) + n : 4 * (EARLY + LATE) + n + 1, :]


def statistics(series, mask, wide):
    middle, early, late = series[EARLY:DEPTH], series[:EARLY], series[DEPTH:]
    first_middle, second_middle = total(middle), total(middle * middle)
    found = []
    for k in range(4):
        days = twice(by_day(mask, k))
        kept_early, kept_late = early * days[:EARLY], late * days[EARLY:]
        first = first_middle + total(kept_early) + total(kept_late)
        second = second_middle + total(kept_early * kept_early) + total(kept_late * kept_late)
        found.append((first, lax.rsqrt((second - first * first / wide) / wide + 1e-06)))
    return found


def along_lanes(table):
    high = table.astype(jnp.bfloat16)
    rest = table - high.astype(jnp.float32)
    middle = rest.astype(jnp.bfloat16)
    low = (rest - middle.astype(jnp.float32)).astype(jnp.bfloat16)
    parts = jnp.concatenate([part.astype(jnp.float32) for part in (high, middle, low)] + [jnp.zeros_like(table)], axis=0)
    row = lax.broadcasted_iota(jnp.int32, (4 * 8, 8 * LANES), 0)
    lane = lax.broadcasted_iota(jnp.int32, (4 * 8, 8 * LANES), 1)
    ones = jnp.where(row % 8 == lane // LANES, 1.0, 0.0).astype(jnp.bfloat16)
    return lax.dot_general(
        parts.astype(jnp.bfloat16), ones, (((0,), (0,)), ((), ())), preferred_element_type=jnp.float32
    )


def prepare_rows(mask, blocks, low, high, spread):
    x, yl = lax.axis_index("x"), lax.axis_index("yl")
    wide = twice(by_slot(mask, 8))
    for step, block in zip((0, 3, 1, 2), blocks):
        rows = pl.ds(pl.multiple_of(lax.rem(x + step, 4) * 256, 256), 256)
        series = days_by_assets(block, yl)
        assets = series.shape[1]
        found = statistics(series, mask, wide)
        turned = along_lanes(jnp.concatenate([first for first, _ in found] + [scale for _, scale in found], axis=0))
        for i in range(8):
            spread[i, rows, :] = turned[:, i * LANES : (i + 1) * LANES]
        high[rows, :] = series[LANES:DEPTH].T.astype(jnp.bfloat16)
        main = series[:LANES].T
        folded = jnp.concatenate([series[DEPTH:], jnp.zeros((LANES - LATE, assets), jnp.float32)], axis=0).T
        for k in range(4):
            left = jnp.where(by_slot(mask, 4 + k) > 0.5, folded, main * by_slot(mask, k))
            low[k, rows, :] = left.astype(jnp.bfloat16)


def correlate(block, mask, low, high, spread, finish):
    half = lax.rem(lax.axis_index("yl") + lax.axis_index("yh") + lax.axis_index("x") // 2, 2)
    wide = twice(by_slot(mask, 8))
    series = days_by_assets(block, half)
    common = series[LATE:DEPTH].astype(jnp.bfloat16)
    for k, (first, scale) in enumerate(statistics(series, mask, wide)):
        mean, scale = first / wide, scale / wide
        head = jnp.where(twice(by_day(mask, k)[EARLY:]) > 0.5, series[DEPTH:], series[:LATE])
        right = jnp.concatenate([head.astype(jnp.bfloat16), common], axis=0)
        for i in range(low.shape[1] // CHUNK):
            rows = slice(i * CHUNK, (i + 1) * CHUNK)
            left = jnp.concatenate([low[k, rows, :], high[rows, :]], axis=1)
            gram = jnp.dot(left, right, preferred_element_type=jnp.float32)
            row_sum, row_scale = spread[k, rows, :], spread[4 + k, rows, :]
            tiles = []
            for h in (slice(0, LANES), slice(LANES, 2 * LANES)):
                cov = gram[:, h] - row_sum * mean[:, h]
                tiles.append((cov * row_scale * scale[:, h]).astype(jnp.bfloat16))
            finish(k, i, rows, tiles)


def columns_of(source):
    x, c, yl, zq = (lax.axis_index(name) for name in ("x", "c", "yl", "zq"))
    step = {"own": 0, "before": 3, "after": 1, "across": 2}[source]
    return pl.ds(pl.multiple_of(lax.rem(x + zq - 2 * c - yl + step + 8, 4) * 256, 256), 256)


def store(result, k, rows, tiles):
    for n, tile in enumerate(tiles):
        result[k, rows, n * LANES : (n + 1) * LANES] = tile


def begin(mask, own, before, after, across, own_block, low, high, spread, result):
    prepare_rows(mask, (own, before, after, across), low, high, spread)

    def finish(k, i, rows, tiles):
        store(result, k, rows, tiles)

    correlate(own_block, mask, low, high, spread, finish)


def go_on(sources, ready, kept, mask, low, high, spread, *refs):
    count = len(sources)
    blocks, held, out = refs[:count], refs[count], refs[-3 - (kept is not None)]
    result, sems = refs[-2:]
    copies = []

    def send(block, number, k, i, rows, source):
        copy = pltpu.make_async_copy(block.at[k, rows], out.at[k, rows, columns_of(source)], sems.at[number, k, i])
        copy.start()
        copies.append(copy)

    for k in range(4):
        for i in range(low.shape[1] // CHUNK):
            send(held, count, k, i, slice(i * CHUNK, (i + 1) * CHUNK), ready)

    def work():
        for n, (source, block) in enumerate(zip(sources, blocks)):

            def finish(k, i, rows, tiles, n=n, source=source):
                store(refs[-3] if source == kept else result.at[n], k, rows, tiles)
                if source != kept:
                    send(result.at[n], n, k, i, rows, source)

            correlate(block, mask, low, high, spread, finish)

    if kept is None:
        work()
    else:
        pl.when(lax.axis_index("x") >= 0)(work)
    for copy in copies:
        copy.wait()


def exchange_and_correlate(returns, window, out_days):
    vmem, anywhere = pl.BlockSpec(memory_space=pltpu.VMEM), pl.BlockSpec(memory_space=pl.ANY)
    assets = 1024
    smem = pl.BlockSpec(memory_space=pltpu.SMEM)
    mask = pl.pallas_call(
        write_masks,
        out_shape=jax.ShapeDtypeStruct((4 * (EARLY + LATE) + 16, LANES), jnp.float32),
        in_specs=[smem, smem],
        out_specs=vmem,
        cost_estimate=pl.CostEstimate(flops=1_000_000_000, bytes_accessed=200_000, transcendentals=0),
        compiler_params=PARAMS,
        name="write_masks",
    )(window, out_days)
    pair = lax.all_gather(returns, "c", axis=0)
    turned = lax.ppermute(pair, AXES, corner_turn())
    own_rows = jnp.stack([pair, lax.ppermute(pair, "yl", ring(2, 1))])
    other = lax.ppermute(turned, "yh", ring(2, 1))
    rows = [own_rows]
    for links in (ring(4, 1), ring(4, 3), ring(4, 2)):
        rows.append(lax.ppermute(own_rows, "x", links))
    own = jnp.stack([turned, other])
    quarters = {"own": own}
    for source, links in (("before", ring(8, 1)), ("after", ring(8, 7)), ("across", two_apart(8))):
        quarters[source] = lax.ppermute(own, ("zh", "zq"), links)

    *prepared, own_result = pl.pallas_call(
        begin,
        out_shape=(
            jax.ShapeDtypeStruct((4, assets, LANES), jnp.bfloat16),
            jax.ShapeDtypeStruct((assets, LANES), jnp.bfloat16),
            jax.ShapeDtypeStruct((8, assets, LANES), jnp.float32),
            jax.ShapeDtypeStruct((4, assets, 256), jnp.bfloat16),
        ),
        in_specs=[vmem] * 6,
        out_specs=(vmem,) * 4,
        cost_estimate=pl.CostEstimate(flops=4_000_000_000, bytes_accessed=4_000_000, transcendentals=0),
        compiler_params=PARAMS,
        name="begin",
    )(mask, *rows, own)
    quarter = jax.ShapeDtypeStruct((4, assets, 256), jnp.bfloat16)
    whole = jax.ShapeDtypeStruct((4, assets, assets), jnp.bfloat16)
    out, ready, held = [], "own", own_result
    for number, sources in enumerate(CALLS):
        count, last = len(sources), number + 1 == len(CALLS)
        out = pl.pallas_call(
            functools.partial(go_on, sources, ready, None if last else sources[-1]),
            out_shape=(whole,) if last else (whole, quarter),
            in_specs=[vmem] * (5 + count) + [anywhere] * len(out),
            out_specs=(anywhere,) if last else (anywhere, vmem),
            scratch_shapes=[
                pltpu.VMEM((count, 4, assets, 256), jnp.bfloat16),
                pltpu.SemaphoreType.DMA((count + 1, 4, assets // CHUNK)),
            ],
            input_output_aliases={5 + count: 0} if out else {},
            cost_estimate=pl.CostEstimate(
                flops=2_000_000_000 * count, bytes_accessed=2_000_000 * count, transcendentals=0
            ),
            compiler_params=pltpu.CompilerParams(vmem_limit_bytes=GRANT),
            name="go_on",
        )(mask, *prepared, *[quarters[source] for source in sources], held, *out)
        ready, out, held = sources[-1], out[:1], out[-1]
    return out[0]


def solution(mesh):
    fine = Mesh(mesh.devices.reshape(SIZES), AXES)
    return jax.shard_map(
        exchange_and_correlate,
        mesh=fine,
        in_specs=(P("yl", ("yh", "zh", "zq", "x", "c")), P(), P()),
        out_specs=P(None, ("yh", "zh", "zq"), ("x", "c", "yl")),
        check_vma=False,
    )
```
